32 devices in a mesh: dp: 16 (over z, y, x), tp: 2 (over core).
Axes of the slice: x: 2, y: 2, z: 4, core: 2. Of those that a mesh axis runs over, the one named last changes fastest.
Arguments:
- tokens: bfloat16 [2048, 4096], P('dp', 'tp'), may hold values from -6 to 6
- norm_gain: float32 [4096], replicated, may hold values from 0.1 to 1.9
- w_query: bfloat16 [4096, 2048], P(None, 'tp'), may hold values from -0.09375 to 0.09375
- w_key: bfloat16 [4096, 512], P(None, 'tp'), may hold values from -0.09375 to 0.09375
- w_value: bfloat16 [4096, 512], P(None, 'tp'), may hold values from -0.09375 to 0.09375
- w_out: bfloat16 [2048, 4096], P('tp'), may hold values from -0.125 to 0.125
- mlp_gain: float32 [4096], replicated, may hold values from 0.1 to 1.9
- w_gate: bfloat16 [4096, 7168], P(None, 'tp'), may hold values from -0.09375 to 0.09375
- w_up: bfloat16 [4096, 7168], P(None, 'tp'), may hold values from -0.09375 to 0.09375
- w_down: bfloat16 [7168, 4096], P('tp'), may hold values from -0.0625 to 0.0625
- kv_pool: bfloat16 [1024, 2, 4, 128, 128], P('dp', None, 'tp'), may hold values from -160 to 160, as said below
- prefix_len: int32 [16], replicated, may hold values from 1024 to 8192, as said below
- page_owner: int32 [16, 64], replicated, may hold values from -1 to 15, as said below
- page_slot: int32 [16, 64], replicated, may hold values from -1 to 63, as said below
- serving: int32 [16], replicated, may hold values from 0 to 15, each once
Outputs:
- context: bfloat16 [2048, 2048], P('dp', 'tp')
- layer_out: bfloat16 [2048, 4096], P('dp', 'tp')
The draws below stay inside these ranges and needn't reach their ends.
Inputs may be any that keep to these rules, and one draw needn't show every extreme that they name: `prefix_len`: prefix lengths lie between 1024 and 8192; some request has exactly 8192 cached tokens and some exactly 1024. page_owner[r, p] names an index along dp for p < ceil(prefix_len[r] / 128) and is -1 after; no index holds more than 4 pages of one request, and for every request some index holds exactly 4 of its pages. page_slot[r, p] lies in 0 to 63 where page_owner[r, p] is not -1 and is -1 where it is; no two pages share the same holder and slot. serving is a permutation of the requests. `kv_pool`: cached keys and values, each page with an offset of its own.
All inputs are finite; a program needn't handle non-finite values.
Results may differ from the reference program's by a relative error of at most 0.014.
The reference program's roundings to bfloat16 on the way count: a program that leaves them out, or rounds other values in their place, can miss the bound.
Values may be sent and summed in bfloat16 or wider, within the bound.
A program may use at most 256 MiB of HBM per device.

```python
import math
import jax
import jax.numpy as jnp
from jax import lax

D = 4096
HD = 128
QH = 16
KVH = 4
FF_WIN = 7168
PAGE = 128
MAXP = 64
NEW = 128
REQUESTS = 16
TOKENS = 2048
SLOTS = 1024
PER_OWNER = 4
N_DP = 16
N_TP = 2


def permute_one(sub_key):
    return jax.random.permutation(sub_key, MAXP)


def layout(key):
    shortest = PAGE * MAXP // 8
    longest = PAGE * MAXP
    lengths = jax.random.randint(jax.random.fold_in(key, 101), (REQUESTS,), shortest, longest + 1)
    top_pick = jax.random.randint(jax.random.fold_in(key, 102), (), 0, REQUESTS)
    low_pick = (top_pick + jax.random.randint(jax.random.fold_in(key, 103), (), 1, REQUESTS)) % REQUESTS
    request_ids = jnp.arange(REQUESTS)
    lengths = jnp.where(request_ids == top_pick, longest, jnp.where(request_ids == low_pick, shortest, lengths))
    page_count = (lengths + PAGE - 1) // PAGE
    shifts = jax.random.permutation(jax.random.fold_in(key, 104), REQUESTS)
    relabel = jax.random.permutation(jax.random.fold_in(key, 105), REQUESTS)
    slot_orders = jax.vmap(permute_one)(jax.random.split(jax.random.fold_in(key, 106), REQUESTS))
    page_ids = jnp.arange(MAXP)
    block_ids = page_ids // PER_OWNER
    owner_spot = (block_ids[None, :] + shifts[:, None]) % REQUESTS
    owners = jnp.take(relabel, owner_spot)
    slot_ids = slot_orders[owners, page_ids[None, :]]
    in_prefix = page_ids[None, :] < page_count[:, None]
    return (lengths.astype(jnp.int32), jnp.where(in_prefix, owners, -1).astype(jnp.int32), jnp.where(in_prefix, slot_ids, -1).astype(jnp.int32))


def draw_prefix_len(key, part):
    return layout(key)[0]


def draw_page_owner(key, part):
    return layout(key)[1]


def draw_page_slot(key, part):
    return layout(key)[2]


def draw_kv_pool(key, part):
    base_key = jax.random.fold_in(key, 7)
    page_key = jax.random.fold_in(key, 8)
    full_shape = (SLOTS, 2, KVH, PAGE, HD)
    page_shape = (SLOTS, 2, KVH, 1, HD)
    base = jax.random.normal(base_key, full_shape, jnp.float32)
    offset = jax.random.normal(page_key, page_shape, jnp.float32)
    return (base + offset).astype(jnp.bfloat16)


def steps_of(key, dims, shards, smallest, largest):
    factor_of, own = 1.0, jax.random.fold_in(key, 6)
    for dim, blocks in shards:
        heights = jnp.exp(jax.random.uniform(jax.random.fold_in(own, dim), (blocks,), jnp.float32, smallest / len(shards), largest / len(shards)))
        factor_of = factor_of * jnp.repeat(heights, dims[dim] // blocks).reshape([-1 if axis == dim else 1 for axis in range(len(dims))])
    return factor_of


def normal_values(stream_key, extent, scale, limit, shards=(), held_as=jnp.bfloat16):
    level = steps_of(stream_key, extent, shards, -0.22, 0.18) if shards else 1.0
    entries = jax.random.normal(stream_key, extent, jnp.float32) * scale * level
    return jnp.minimum(jnp.maximum(entries, -limit), limit).astype(held_as)


def setup_inputs(seed: int = 0) -> dict:
    arg_keys = jax.random.split(jax.random.key(seed), 16)
    tokens = normal_values(arg_keys[0], (TOKENS, D), 1.0, 6.0, ((0, 16), (1, 2)))
    norm_gain = jnp.clip(1.0 + 0.18 * jax.random.normal(arg_keys[1], (D,), jnp.float32), 0.1, 1.9)
    w_query = normal_values(arg_keys[2], (D, QH * HD), D ** -0.5, 0.09375, ((1, 2),))
    w_key = normal_values(arg_keys[3], (D, KVH * HD), D ** -0.5, 0.09375, ((1, 2),))
    w_value = normal_values(arg_keys[4], (D, KVH * HD), D ** -0.5, 0.09375, ((1, 2),))
    w_out = normal_values(arg_keys[5], (QH * HD, D), (QH * HD) ** -0.5, 0.125, ((0, 2),))
    mlp_gain = jnp.clip(1.0 + 0.18 * jax.random.normal(arg_keys[6], (D,), jnp.float32), 0.1, 1.9)
    w_gate = normal_values(arg_keys[7], (D, FF_WIN), D ** -0.5, 0.09375, ((1, 2),))
    w_up = normal_values(arg_keys[8], (D, FF_WIN), D ** -0.5, 0.09375, ((1, 2),))
    w_down = normal_values(arg_keys[9], (FF_WIN, D), FF_WIN ** -0.5, 0.0625, ((0, 2),))
    kv_pool = draw_kv_pool(jax.random.fold_in(arg_keys[15], 71), 0)
    prefix_len = draw_prefix_len(jax.random.fold_in(arg_keys[15], 71), 0)
    page_owner = draw_page_owner(jax.random.fold_in(arg_keys[15], 71), 0)
    page_slot = draw_page_slot(jax.random.fold_in(arg_keys[15], 71), 0)
    serving = jax.random.permutation(arg_keys[14], REQUESTS).astype(jnp.int32)
    return {"tokens": tokens, "norm_gain": norm_gain, "w_query": w_query, "w_key": w_key, "w_value": w_value, "w_out": w_out, "mlp_gain": mlp_gain, "w_gate": w_gate, "w_up": w_up, "w_down": w_down, "kv_pool": kv_pool, "prefix_len": prefix_len, "page_owner": page_owner, "page_slot": page_slot, "serving": serving}


EPS = 1e-05
THETA = 500000.0
NEG = -1e+30

def rms_normalize(values, gain):
    as_f32 = values.astype(jnp.float32)
    factor = lax.rsqrt(lax.optimization_barrier(jnp.mean(as_f32 * as_f32, axis=-1, keepdims=True)) + EPS)
    return (as_f32 * factor * gain).astype(jnp.bfloat16)

def rotate(vectors, positions):
    half_dim = vectors.shape[-1] // 2
    freq_index = jnp.arange(half_dim, dtype=jnp.float32)
    inverse = jnp.power(jnp.float32(THETA), -2.0 * freq_index / vectors.shape[-1])
    angles = positions.astype(jnp.float32)[:, None] * inverse[None, :]
    cosine = jnp.cos(angles)[:, None, :]
    sine = jnp.sin(angles)[:, None, :]
    first = vectors[..., :half_dim]
    second = vectors[..., half_dim:]
    return jnp.concatenate([first * cosine - second * sine, second * cosine + first * sine], axis=-1)

def attend(queries, keys_all, values_all, length, new_tokens):
    row_count = queries.shape[1]
    prefix_slots = keys_all.shape[1] - new_tokens
    scores = jnp.einsum('hqd,hkd->hqk', queries.astype(jnp.float32), keys_all.astype(jnp.float32))
    scores = scores / math.sqrt(queries.shape[2])
    row_token = jnp.arange(row_count, dtype=jnp.int32) % new_tokens
    prefix_ok = jnp.arange(prefix_slots, dtype=jnp.int32) < length
    causal = jnp.arange(new_tokens, dtype=jnp.int32)[None, :] <= row_token[:, None]
    allowed = jnp.concatenate([jnp.broadcast_to(prefix_ok[None, :], (row_count, prefix_slots)), causal], axis=1)
    scores = jnp.where(allowed[None], scores, NEG)
    highest = lax.optimization_barrier(jnp.max(scores, axis=-1, keepdims=True))
    expo = jnp.exp(scores - highest)
    weights = (expo / lax.optimization_barrier(jnp.sum(expo, axis=-1, keepdims=True))).astype(jnp.bfloat16)
    result = jnp.einsum('hqk,hkd->hqd', weights.astype(jnp.float32), values_all.astype(jnp.float32))
    return result.astype(jnp.bfloat16)

def rounded_blocks(left, right, blocks):
    block_size = left.shape[1] // blocks
    running = jnp.zeros((left.shape[0], right.shape[1]), jnp.float32)
    for index in range(blocks):
        partial_sum = jnp.dot(left[:, index * block_size:(index + 1) * block_size], right[index * block_size:(index + 1) * block_size], preferred_element_type=jnp.float32)
        partial_sum = lax.optimization_barrier(partial_sum.astype(jnp.bfloat16))
        running = running + partial_sum.astype(jnp.float32)
    return running

def reference(tokens, norm_gain, w_query, w_key, w_value, w_out, mlp_gain, w_gate, w_up, w_down, kv_pool, prefix_len, page_owner, page_slot, serving):
    normed = rms_normalize(tokens, norm_gain)
    starts = jnp.take(prefix_len, serving.astype(jnp.int32))
    positions = (starts[:, None] + jnp.arange(NEW, dtype=jnp.int32)[None, :]).reshape(-1)
    queries = rotate(jnp.dot(normed, w_query, preferred_element_type=jnp.float32).reshape(TOKENS, QH, HD), positions).astype(jnp.bfloat16)
    new_keys = rotate(jnp.dot(normed, w_key, preferred_element_type=jnp.float32).reshape(TOKENS, KVH, HD), positions).astype(jnp.bfloat16)
    new_values = jnp.dot(normed, w_value, preferred_element_type=jnp.float32).astype(jnp.bfloat16).reshape(TOKENS, KVH, HD)
    shared = QH // KVH

    def one_group(items):
        group_q, group_k, group_v, request = items
        length = prefix_len[request]
        owner_row = page_owner[request]
        slot_row = page_slot[request]
        row_index = jnp.where(owner_row >= 0, owner_row * MAXP + slot_row, 0).astype(jnp.int32)
        pages = jnp.take(kv_pool, row_index, axis=0)
        keys_all = jnp.concatenate([pages[:, 0].transpose(1, 0, 2, 3).reshape(KVH, MAXP * PAGE, HD), group_k.transpose(1, 0, 2)], axis=1)
        values_all = jnp.concatenate([pages[:, 1].transpose(1, 0, 2, 3).reshape(KVH, MAXP * PAGE, HD), group_v.transpose(1, 0, 2)], axis=1)
        stacked = group_q.reshape(NEW, KVH, shared, HD).transpose(1, 2, 0, 3).reshape(KVH, shared * NEW, HD)
        result = attend(stacked, keys_all, values_all, length, NEW)
        return result.reshape(KVH, shared, NEW, HD).transpose(2, 0, 1, 3).reshape(NEW, QH * HD)
    context = lax.map(one_group, (queries.reshape(N_DP, NEW, QH, HD), new_keys.reshape(N_DP, NEW, KVH, HD), new_values.reshape(N_DP, NEW, KVH, HD), serving.astype(jnp.int32)))
    context = context.reshape(TOKENS, QH * HD)
    attn_sum = rounded_blocks(context, w_out, N_TP)
    stream = (tokens.astype(jnp.float32) + attn_sum).astype(jnp.bfloat16)
    mlp_in = rms_normalize(stream, mlp_gain)
    gate_act = jnp.dot(mlp_in, w_gate, preferred_element_type=jnp.float32)
    up_act = jnp.dot(mlp_in, w_up, preferred_element_type=jnp.float32)
    hidden = (jax.nn.silu(gate_act) * up_act).astype(jnp.bfloat16)
    mlp_sum = rounded_blocks(hidden, w_down, N_TP)
    layer_out = (stream.astype(jnp.float32) + mlp_sum).astype(jnp.bfloat16)
    return (context, layer_out)
```

```python
import functools
import math

import jax
import jax.numpy as jnp
from jax import lax
from jax.experimental import pallas as pl
from jax.experimental.pallas import tpu as pltpu
from jax.sharding import PartitionSpec as P

EPS = 1e-05
THETA = 500000.0
NEG = -1e30
MESH = pl.DeviceIdType.MESH
VMEM = pltpu.VMEM


def rotate(vectors, positions):
    half_dim = vectors.shape[-1] // 2
    freq_index = jnp.arange(half_dim, dtype=jnp.float32)
    inverse = jnp.power(jnp.float32(THETA), -2.0 * freq_index / vectors.shape[-1])
    angles = positions.astype(jnp.float32)[:, None] * inverse[None, :]
    cosine = jnp.cos(angles)[:, None, :]
    sine = jnp.sin(angles)[:, None, :]
    first = vectors[..., :half_dim]
    second = vectors[..., half_dim:]
    return jnp.concatenate(
        [first * cosine - second * sine, second * cosine + first * sine], axis=-1
    )


def bit_orders(levels):
    down = list(range(levels - 1, -1, -1))
    swapped = down[:-2] + [down[-1], down[-2]]
    low_first = [0, 1] + list(range(levels - 1, 1, -1))
    return [down, swapped, low_first]


def head_groups(heads):
    first = (heads + 2) // 3
    second = (heads - first + 1) // 2
    sizes = [first, second, heads - first - second]
    starts = [0, first, first + second]
    return list(zip(starts, sizes))


def span(bits):
    masks = [0]
    for bit in bits:
        masks = masks + [mask | (1 << bit) for mask in masks]
    return masks


def flipped(me, mask):
    out = me
    bit = 0
    while (1 << bit) <= mask:
        if mask & (1 << bit):
            out = out + (1 - 2 * (lax.rem(me // (1 << bit), 2))) * (1 << bit)
        bit += 1
    return out


def greet(levels, me):
    barrier = pltpu.get_barrier_semaphore()
    for bit in range(levels):
        pl.semaphore_signal(
            barrier, inc=1, device_id={"dp": flipped(me, 1 << bit)}, device_id_type=MESH
        )
    pl.semaphore_wait(barrier, levels)


def gather_kernel(levels, q_ref, out_ref, send_sem, recv_sem, own_sem):
    me = lax.axis_index("dp")
    greet(levels, me)
    groups = head_groups(q_ref.shape[0])
    orders = bit_orders(levels)
    sends = []
    own = pltpu.make_async_copy(q_ref, out_ref.at[me], own_sem)
    own.start()

    def copy_of(piece, mask, bit):
        start, size = groups[piece]
        block = flipped(me, mask)
        heads = pl.ds(start, size)
        key = mask | (1 << bit)
        source = q_ref.at[heads] if mask == 0 else out_ref.at[block, heads]
        return pltpu.make_async_remote_copy(
            src_ref=source,
            dst_ref=out_ref.at[block, heads],
            send_sem=send_sem.at[piece, key],
            recv_sem=recv_sem.at[piece, key],
            device_id={"dp": flipped(me, 1 << bit)},
            device_id_type=MESH,
        )

    def wait_arrival(piece, mask):
        start, size = groups[piece]
        landed = out_ref.at[flipped(me, mask), pl.ds(start, size)]
        pltpu.make_async_copy(landed, landed, recv_sem.at[piece, mask]).wait()

    for level in range(levels):
        for index in range(1 << level):
            for piece in range(3):
                if groups[piece][1] == 0:
                    continue
                order = orders[piece]
                mask = span(order[:level])[index]
                if mask and index >= (1 << (level - 1)):
                    wait_arrival(piece, mask)
                copy = copy_of(piece, mask, order[level])
                copy.start()
                sends.append(copy)
    for piece in range(3):
        if groups[piece][1]:
            for mask in span(orders[piece])[1 << (levels - 1) :]:
                wait_arrival(piece, mask)
    for copy in sends:
        copy.wait_send()
    own.wait()


def attend_kernel(
    per_owner, slot_ref, valid_ref, q_ref, kv_ref, nk_ref, nv_ref, part_ref, stat_ref
):
    me = lax.axis_index("dp")
    total, heads, rows, width = q_ref.shape
    kv_heads = kv_ref.shape[2]
    page = kv_ref.shape[3]
    shared = heads // kv_heads
    scale = 1.0 / math.sqrt(width)
    stat_row = lax.broadcasted_iota(jnp.int32, (8, rows), 0)

    def scores_of(keys, group, kv_head):
        queries = q_ref[group, kv_head * shared : (kv_head + 1) * shared]
        queries = queries.reshape(shared * rows, width)
        return (
            lax.dot_general(
                keys, queries, (((1,), (1,)), ((), ())), preferred_element_type=jnp.float32
            )
            * scale
        )

    def summed(scores, values):
        highest = jnp.max(scores, axis=0, keepdims=True)
        expo = jnp.exp(scores - highest)
        total_of = jnp.sum(expo, axis=0, keepdims=True)
        part = lax.dot_general(
            values,
            expo.astype(jnp.bfloat16),
            (((0,), (0,)), ((), ())),
            preferred_element_type=jnp.float32,
        )
        return highest, total_of, part

    def stats(highest, total_of):
        return jnp.where(stat_row < 4, highest, total_of)

    def one_group(group, carry):
        held = valid_ref[group, 0] > 0

        @pl.when(held)
        def _():
            row = lax.broadcasted_iota(jnp.int32, (page, 1), 0)
            ok = jnp.concatenate(
                [row < valid_ref[group, k] for k in range(per_owner)], axis=0
            )
            for kv_head in range(kv_heads):
                keys = jnp.concatenate(
                    [kv_ref[slot_ref[group, k], 0, kv_head] for k in range(per_owner)], axis=0
                )
                values = jnp.concatenate(
                    [kv_ref[slot_ref[group, k], 1, kv_head] for k in range(per_owner)], axis=0
                )
                scores = jnp.where(ok, scores_of(keys, group, kv_head), NEG)
                highest, total_of, part = summed(scores, values)
                for j in range(shared):
                    lanes = slice(j * rows, (j + 1) * rows)
                    part_ref[group, kv_head * shared + j] = part[:, lanes].astype(jnp.bfloat16)
                    stat_ref[group, kv_head * shared + j] = stats(
                        highest[:, lanes], total_of[:, lanes]
                    )

        @pl.when(jnp.logical_not(held))
        def _():
            for head in range(heads):
                part_ref[group, head] = jnp.zeros((width, rows), jnp.bfloat16)
                stat_ref[group, head] = jnp.where(stat_row < 4, NEG, 0.0)

        return carry

    lax.fori_loop(0, total, one_group, 0)

    key_row = lax.broadcasted_iota(jnp.int32, (rows, shared * rows), 0)
    token = lax.rem(lax.broadcasted_iota(jnp.int32, (rows, shared * rows), 1), rows)
    for kv_head in range(kv_heads):
        scores = jnp.where(key_row <= token, scores_of(nk_ref[kv_head], me, kv_head), NEG)
        highest, total_of, part = summed(scores, nv_ref[kv_head])
        for j in range(shared):
            head = kv_head * shared + j
            lanes = slice(j * rows, (j + 1) * rows)
            before = stat_ref[me, head]
            top, count, summed_part = merge(
                before[0:1],
                before[4:5],
                part_ref[me, head].astype(jnp.float32),
                highest[:, lanes],
                total_of[:, lanes],
                part[:, lanes],
            )
            part_ref[me, head] = summed_part.astype(jnp.bfloat16)
            stat_ref[me, head] = stats(top, count)


def merge(top_a, count_a, part_a, top_b, count_b, part_b):
    top = jnp.maximum(top_a, top_b)
    factor_a = jnp.exp(top_a - top)
    factor_b = jnp.exp(top_b - top)
    return (
        top,
        count_a * factor_a + count_b * factor_b,
        part_a * factor_a + part_b * factor_b,
    )


def home_kernel(
    levels, part_ref, stat_ref, out_ref, part_box, stat_box, part_send, part_recv, stat_send, stat_recv
):
    me = lax.axis_index("dp")
    greet(levels, me)
    heads, width, rows = part_ref.shape[1:]
    groups = head_groups(heads)
    orders = [order[::-1] for order in bit_orders(levels)]
    stat_row = lax.broadcasted_iota(jnp.int32, (8, rows), 0)
    sends = []
    where = {}

    def held(piece, mask):
        if (piece, mask) in where:
            key = where[piece, mask]
            return part_box.at[key], stat_box.at[key]
        block = flipped(me, mask)
        return part_ref.at[block], stat_ref.at[block]

    def send(piece, level, mask):
        order = orders[piece]
        bit = 1 << order[level]
        cut = pl.ds(*groups[piece])
        part, stat = held(piece, mask)
        for source, box, out_sem, in_sem in (
            (part, part_box, part_send, part_recv),
            (stat, stat_box, stat_send, stat_recv),
        ):
            copy = pltpu.make_async_remote_copy(
                src_ref=source.at[cut],
                dst_ref=box.at[mask, cut],
                send_sem=out_sem.at[piece, mask],
                recv_sem=in_sem.at[piece, mask],
                device_id={"dp": flipped(me, bit)},
                device_id_type=MESH,
            )
            copy.start()
            sends.append(copy)

    def take(piece, level, mask):
        order = orders[piece]
        key = mask | (1 << order[level])
        start, size = groups[piece]
        cut = pl.ds(start, size)
        part, stat = held(piece, mask)
        for box, in_sem in ((part_box, part_recv), (stat_box, stat_recv)):
            landed = box.at[key, cut]
            pltpu.make_async_copy(landed, landed, in_sem.at[piece, key]).wait()
        last = level == levels - 1

        def one_head(head):
            mine = stat[head]
            came = stat_box[key, head]
            top, count, merged = merge(
                mine[0:1],
                mine[4:5],
                part[head].astype(jnp.float32),
                came[0:1],
                came[4:5],
                part_box[key, head].astype(jnp.float32),
            )
            return top, count, merged

        if last:
            for head in range(start, start + size):
                _, count, merged = one_head(head)
                out_ref[:, head * width : (head + 1) * width] = (merged / count).T.astype(
                    out_ref.dtype
                )
        else:

            def body(head, carry):
                top, count, merged = one_head(head)
                part_box[key, head] = merged.astype(jnp.bfloat16)
                stat_box[key, head] = jnp.where(stat_row < 4, top, count)
                return carry

            lax.fori_loop(start, start + size, body, 0)
            where[piece, mask] = key

    live = [piece for piece in range(3) if groups[piece][1]]
    for index in range(1 << (levels - 1)):
        for piece in live:
            order = orders[piece]
            send(piece, 0, span(order[:0:-1])[index] | (1 << order[0]))
    for level in range(levels):
        if level == levels - 1:
            for piece in live:
                take(piece, level, 0)
            break
        for forward in (True, False):
            for index in range(1 << (levels - 2 - level)):
                for piece in live:
                    order = orders[piece]
                    mask = span(order[: level + 1 : -1])[index]
                    if forward:
                        mask = mask | (1 << order[level + 1])
                    take(piece, level, mask)
                    if forward:
                        send(piece, level + 1, mask)
    for copy in sends:
        copy.wait_send()


def attention(queries, new_keys, new_values, kv_pool, slot_pick, valid, groups, per_owner):
    heads, rows, width = queries.shape
    levels = groups.bit_length() - 1
    vmem = pl.BlockSpec(memory_space=VMEM)
    smem = pl.BlockSpec(memory_space=pltpu.SMEM)
    dma = pltpu.SemaphoreType.DMA
    all_queries = pl.pallas_call(
        functools.partial(gather_kernel, levels),
        out_shape=jax.ShapeDtypeStruct((groups, heads, rows, width), jnp.bfloat16),
        in_specs=[vmem],
        out_specs=vmem,
        scratch_shapes=[dma((3, groups)), dma((3, groups)), dma],
        compiler_params=pltpu.CompilerParams(collective_id=0, has_side_effects=True),
        name="query_gather",
    )(queries)
    parts, stats = pl.pallas_call(
        functools.partial(attend_kernel, per_owner),
        out_shape=(
            jax.ShapeDtypeStruct((groups, heads, width, rows), jnp.bfloat16),
            jax.ShapeDtypeStruct((groups, heads, 8, rows), jnp.float32),
        ),
        in_specs=[smem, smem, vmem, vmem, vmem, vmem],
        out_specs=(vmem, vmem),
        name="page_attend",
    )(slot_pick, valid, all_queries, kv_pool, new_keys, new_values)
    return pl.pallas_call(
        functools.partial(home_kernel, levels),
        out_shape=jax.ShapeDtypeStruct((rows, heads * width), jnp.bfloat16),
        in_specs=[vmem, vmem],
        out_specs=vmem,
        scratch_shapes=[
            pltpu.VMEM((groups, heads, width, rows), jnp.bfloat16),
            pltpu.VMEM((groups, heads, 8, rows), jnp.float32),
            dma((3, groups)),
            dma((3, groups)),
            dma((3, groups)),
            dma((3, groups)),
        ],
        compiler_params=pltpu.CompilerParams(collective_id=1, has_side_effects=True),
        name="context_home",
    )(parts, stats)


def shards(
    tokens,
    norm_gain,
    w_query,
    w_key,
    w_value,
    w_out,
    mlp_gain,
    w_gate,
    w_up,
    w_down,
    kv_pool,
    prefix_len,
    page_owner,
    page_slot,
    serving,
):
    groups = lax.axis_size("dp")
    device = lax.axis_index("dp")
    tp_rank = lax.axis_index("tp")
    new_tokens = tokens.shape[0]
    share_width = tokens.shape[1]
    model_width = mlp_gain.shape[0]
    pages_max = page_owner.shape[1]
    per_owner = (pages_max + groups - 1) // groups
    page_len = kv_pool.shape[3]
    head_dim = kv_pool.shape[4]
    kv_heads = kv_pool.shape[2]
    q_heads = w_query.shape[1] // head_dim
    group_ids = jnp.arange(groups, dtype=jnp.int32)
    request = jnp.sum(jnp.where(group_ids == device, serving, 0))
    length = jnp.sum(jnp.where(group_ids == request, prefix_len, 0))
    gathered = lax.all_gather(tokens, "tp", axis=1, tiled=True)
    gathered_f32 = gathered.astype(jnp.float32)
    in_scale = lax.rsqrt(jnp.mean(gathered_f32 * gathered_f32, axis=-1, keepdims=True) + EPS)
    normed = (gathered_f32 * in_scale * norm_gain).astype(jnp.bfloat16)
    positions = length + jnp.arange(new_tokens, dtype=jnp.int32)
    queries = rotate(
        jnp.dot(normed, w_query, preferred_element_type=jnp.float32).reshape(
            new_tokens, q_heads, head_dim
        ),
        positions,
    ).astype(jnp.bfloat16)
    new_keys = rotate(
        jnp.dot(normed, w_key, preferred_element_type=jnp.float32).reshape(
            new_tokens, kv_heads, head_dim
        ),
        positions,
    ).astype(jnp.bfloat16)
    new_values = (
        jnp.dot(normed, w_value, preferred_element_type=jnp.float32)
        .astype(jnp.bfloat16)
        .reshape(new_tokens, kv_heads, head_dim)
    )
    owner_dest = jnp.take(page_owner, serving, axis=0)
    slot_dest = jnp.take(page_slot, serving, axis=0)
    length_dest = jnp.take(prefix_len, serving)
    page_ids = jnp.arange(pages_max, dtype=jnp.int32)
    owned = owner_dest == device
    rank = jnp.cumsum(owned.astype(jnp.int32), axis=1) - 1
    valid_dest = jnp.clip(length_dest[:, None] - page_ids[None, :] * page_len, 0, page_len)
    choose = jnp.arange(per_owner, dtype=jnp.int32)
    picked = owned[:, None, :] & (rank[:, None, :] == choose[None, :, None])
    slot_pick = jnp.sum(jnp.where(picked, slot_dest[:, None, :], 0), axis=2)
    valid = jnp.sum(jnp.where(picked, valid_dest[:, None, :], 0), axis=2)
    context = attention(
        queries.transpose(1, 0, 2),
        new_keys.transpose(1, 0, 2),
        new_values.transpose(1, 0, 2),
        kv_pool,
        slot_pick,
        valid,
        groups,
        per_owner,
    )
    projected = jnp.dot(context, w_out, preferred_element_type=jnp.float32)
    col_start = tp_rank * share_width
    attn_own = lax.psum_scatter(
        projected.astype(jnp.bfloat16), "tp", scatter_dimension=1, tiled=True
    ).astype(jnp.float32)
    stream_own = (tokens.astype(jnp.float32) + attn_own).astype(jnp.bfloat16)
    own_f32 = stream_own.astype(jnp.float32)
    square_total = lax.psum(jnp.sum(own_f32 * own_f32, axis=-1), "tp")
    gain_own = lax.dynamic_slice_in_dim(mlp_gain, col_start, share_width, 0)
    mid_scale = lax.rsqrt(square_total / model_width + EPS)
    normed_share = (own_f32 * mid_scale[:, None] * gain_own).astype(jnp.bfloat16)
    mlp_in = lax.all_gather(normed_share, "tp", axis=1, tiled=True)
    gate_act = jnp.dot(mlp_in, w_gate, preferred_element_type=jnp.float32)
    up_act = jnp.dot(mlp_in, w_up, preferred_element_type=jnp.float32)
    hidden = (jax.nn.silu(gate_act) * up_act).astype(jnp.bfloat16)
    down_part = jnp.dot(hidden, w_down, preferred_element_type=jnp.float32)
    mlp_own = lax.psum_scatter(
        down_part.astype(jnp.bfloat16), "tp", scatter_dimension=1, tiled=True
    ).astype(jnp.float32)
    layer_out = (stream_own.astype(jnp.float32) + mlp_own).astype(jnp.bfloat16)
    return (context, layer_out)


def solution(mesh):
    in_specs = (
        P("dp", "tp"),
        P(),
        P(None, "tp"),
        P(None, "tp"),
        P(None, "tp"),
        P("tp", None),
        P(),
        P(None, "tp"),
        P(None, "tp"),
        P("tp", None),
        P("dp", None, "tp", None, None),
        P(),
        P(),
        P(),
        P(),
    )
    out_specs = (P("dp", "tp"), P("dp", "tp"))
    return jax.shard_map(shards, mesh=mesh, in_specs=in_specs, out_specs=out_specs, check_vma=False)
```
